8 devices in a mesh: dp: 1 (over z), sp: 8 (over x, y, core).
Axes of the slice: x: 2, y: 2, z: 1, core: 2. Of those that a mesh axis runs over, the one named last changes fastest.
Arguments:
- q: bfloat16 [32, 8, 256], P('dp')
- k: bfloat16 [32, 4096, 8, 256], P('dp', 'sp')
- v: bfloat16 [32, 4096, 8, 256], P('dp', 'sp')
Outputs:
- q: bfloat16 [32, 8, 256], P('dp')
All inputs are finite; a program needn't handle non-finite values.
Results may differ from the reference program's by a relative error of at most 0.012.
Values are sent between devices in bfloat16 or wider.
A program may use at most 2 GiB of HBM per device.

```python
import jax
import jax.numpy as jnp

BATCH = 32
CACHE = 4096
HEADS = 8
KV_HEADS = 8
HEAD = 256


def setup_inputs(seed: int = 0, part: int = 0) -> dict:
    kq, kk, kv = (jax.random.fold_in(k, part) for k in jax.random.split(jax.random.key(seed), 3))
    return {
        "q": (3 * jax.random.normal(kq, (BATCH, HEADS, HEAD), jnp.float32)).astype(jnp.bfloat16),
        "k": jax.random.normal(kk, (BATCH, CACHE, KV_HEADS, HEAD), jnp.float32).astype(jnp.bfloat16),
        "v": jax.random.normal(kv, (BATCH, CACHE, KV_HEADS, HEAD), jnp.float32).astype(jnp.bfloat16),
    }


def einsum(form, a, b):
    return jnp.einsum(form, a.astype(jnp.float32), b.astype(jnp.float32))


def reference(q, k, v):
    grouped = q.reshape(BATCH, KV_HEADS, -1, HEAD)
    scores = einsum("bgsd,bugd->bgsu", grouped, k) * HEAD**-0.5
    weights = jax.nn.softmax(scores, -1).astype(jnp.bfloat16)
    return einsum("bgsu,bugd->bgsd", weights, v).astype(jnp.bfloat16).reshape(BATCH, HEADS, HEAD)
```

```python
import functools
import math

import jax
import jax.numpy as jnp
from jax import lax
from jax.experimental import pallas as pl
from jax.experimental.pallas import tpu as pltpu
from jax.sharding import PartitionSpec as P

SLOTS = 3
TILE = 256
LANES = 128


def peers_of(me):
    x, y, core = me // 4, (me // 2) % 2, me % 2
    for dx, dy, dc in ((1, 1, 1), (1, 1, 0), (1, 0, 1), (1, 0, 0), (0, 1, 1), (0, 1, 0), (0, 0, 1)):
        px = 1 - x if dx else x
        py = 1 - y if dy else y
        pc = 1 - core if dc else core
        yield px * 4 + py * 2 + pc


def kernel(n, q_hbm, k_hbm, v_hbm, o_ref, q_buf, k_buf, v_buf, p_buf, parts, stats, q_sem, k_sem, v_sem, send_sem, recv_sem):
    seqs, rows, head = k_hbm.shape
    heads = q_hbm.shape[1]
    tiles = rows // TILE
    log2e_scaled = math.log2(math.e) * head**-0.5
    me = lax.axis_index("sp")
    peers = list(peers_of(me))

    def k_copy(b):
        slot = lax.rem(b, SLOTS)
        return pltpu.make_async_copy(k_hbm.at[b], k_buf.at[slot], k_sem.at[slot])

    def v_copy(b):
        slot = lax.rem(b, SLOTS)
        return pltpu.make_async_copy(v_hbm.at[b], v_buf.at[slot], v_sem.at[slot])

    def to(peer, ref, send, recv):
        return pltpu.make_async_remote_copy(
            src_ref=ref, dst_ref=ref, send_sem=send, recv_sem=recv, device_id={"sp": peer}, device_id_type=pl.DeviceIdType.MESH
        )

    pltpu.make_async_copy(q_hbm, q_buf, q_sem).start()
    k_copy(0).start()
    for b in range(1, SLOTS):
        k_copy(b).start()
        v_copy(b - 1).start()
    v_copy(SLOTS - 1).start()

    barrier = pltpu.get_barrier_semaphore()
    for peer in peers:
        pl.semaphore_signal(barrier, inc=1, device_id={"sp": peer}, device_id_type=pl.DeviceIdType.MESH)

    own = lax.broadcasted_iota(jnp.int32, (heads, TILE), 1) % heads == lax.broadcasted_iota(jnp.int32, (heads, TILE), 0)
    lane = lax.broadcasted_iota(jnp.int32, (heads, LANES), 1)

    def weigh(b, stat):
        slot = lax.rem(b, SLOTS)
        q = q_buf[b]
        scores = []
        for t in range(tiles):
            s = lax.dot_general(q, k_buf[slot, t * TILE : (t + 1) * TILE, :], (((1,), (1,)), ((), ())), preferred_element_type=jnp.float32)
            scores.append(jnp.where(own, s, -jnp.inf))
        high = jnp.max(functools.reduce(jnp.maximum, scores), -1, keepdims=True)
        total = None
        for t in range(tiles):
            w = jnp.exp2((scores[t] - high) * log2e_scaled)
            p_buf[:, t * TILE : (t + 1) * TILE] = w.astype(jnp.bfloat16)
            total = w if total is None else total + w
        total = jnp.sum(total, -1, keepdims=True)
        return jnp.where(lane == b, high, jnp.where(lane == b + LANES // 2, total, stat))

    def gather_values(b):
        slot = lax.rem(b, SLOTS)
        acc = None
        for t in range(tiles):
            d = jnp.dot(p_buf[:, t * TILE : (t + 1) * TILE], v_buf[slot, t * TILE : (t + 1) * TILE, :], preferred_element_type=jnp.float32)
            acc = d if acc is None else acc + d
        parts[me, b] = acc.astype(jnp.bfloat16)

    pltpu.make_async_copy(q_hbm, q_buf, q_sem).wait()
    k_copy(0).wait()
    stat = weigh(0, jnp.zeros((heads, LANES), jnp.float32))
    k_copy(SLOTS).start()

    def step(more_k, more_v, b, stat):
        k_copy(b + 1).wait()
        v_copy(b).wait()
        gather_values(b)
        stat = weigh(b + 1, stat)
        if more_v:
            v_copy(b + SLOTS).start()
        if more_k:
            k_copy(b + 1 + SLOTS).start()
        return stat

    def send(first, count, k):
        for peer in peers:
            to(peer, parts.at[me, first : first + count], send_sem.at[k], recv_sem.at[k]).start()

    begin = 0
    for end in (seqs // 4, seqs // 2, 3 * seqs // 4, seqs - 1 - SLOTS):
        stat = lax.fori_loop(begin, end, functools.partial(step, True, True), stat)
        if begin == 0:
            pl.semaphore_wait(barrier, n - 1)
        send(begin, end - begin, 0)
        begin = end
    stat = step(False, True, begin, stat)
    for b in range(begin + 1, seqs - 1):
        stat = step(False, False, b, stat)
    stats[me] = stat
    send(begin, seqs - 1 - begin, 0)
    for peer in peers:
        to(peer, stats.at[me], send_sem.at[1], recv_sem.at[1]).start()
    v_copy(seqs - 1).wait()
    gather_values(seqs - 1)
    send(seqs - 1, 1, 2)

    to(peers[0], stats.at[0 : n - 1], send_sem.at[1], recv_sem.at[1]).wait()
    seen = [stats[i] for i in range(n)]
    high = functools.reduce(jnp.maximum, seen)
    scale = [jnp.exp2((s - high) * log2e_scaled) for s in seen]
    total = sum(c * pltpu.roll(s, LANES // 2, 1) for c, s in zip(scale, seen))
    scale = [c / total for c in scale]

    def put(b):
        o_ref[b] = sum(scale[i][:, b : b + 1] * parts[i, b].astype(jnp.float32) for i in range(n)).astype(o_ref.dtype)

    to(peers[0], parts.at[0 : n - 1, 0 : seqs - 1], send_sem.at[0], recv_sem.at[0]).wait()
    for b in range(seqs - 1):
        put(b)
    to(peers[0], parts.at[0 : n - 1, 0], send_sem.at[2], recv_sem.at[2]).wait()
    put(seqs - 1)


def solution(mesh):
    n = mesh.shape["sp"]

    def step(q, k, v):
        seqs, tokens, heads, head = k.shape
        rows = tokens * heads
        return pl.pallas_call(
            functools.partial(kernel, n),
            out_shape=pltpu.VMEM(q.shape, q.dtype),
            in_specs=[pl.BlockSpec(memory_space=pl.ANY)] * 3,
            out_specs=pl.BlockSpec(memory_space=pltpu.VMEM),
            scratch_shapes=[
                pltpu.VMEM(q.shape, q.dtype),
                pltpu.VMEM((SLOTS, rows, head), k.dtype),
                pltpu.VMEM((SLOTS, rows, head), v.dtype),
                pltpu.VMEM((heads, rows), jnp.bfloat16),
                pltpu.VMEM((n, seqs, heads, head), jnp.bfloat16),
                pltpu.VMEM((n, heads, LANES), jnp.float32),
                pltpu.SemaphoreType.DMA,
                pltpu.SemaphoreType.DMA((SLOTS,)),
                pltpu.SemaphoreType.DMA((SLOTS,)),
                pltpu.SemaphoreType.DMA((3,)),
                pltpu.SemaphoreType.DMA((3,)),
            ],
            compiler_params=pltpu.CompilerParams(collective_id=0, has_side_effects=True),
        )(q, k.reshape(seqs, rows, head), v.reshape(seqs, rows, head))

    return jax.shard_map(
        step,
        mesh=mesh,
        in_specs=(P("dp", None, None), P("dp", "sp", None, None), P("dp", "sp", None, None)),
        out_specs=P("dp", None, None),
        check_vma=False,
    )
```

```python
import functools
import math

import jax
import jax.numpy as jnp
from jax import lax
from jax.experimental import pallas as pl
from jax.experimental.pallas import tpu as pltpu
from jax.sharding import PartitionSpec as P

K_SLOTS, V_SLOTS = 5, 7
FLIGHT = 5
LEAD = 3
PIECES = 1
TILE = 256
LANES = 128


def peers_of(me):
    x, y, core = me // 4, (me // 2) % 2, me % 2
    for dx, dy, dc in ((1, 1, 0), (1, 1, 1), (1, 0, 0), (1, 0, 1), (0, 1, 0), (0, 1, 1), (0, 0, 1)):
        px = 1 - x if dx else x
        py = 1 - y if dy else y
        pc = 1 - core if dc else core
        yield px * 4 + py * 2 + pc


def kernel(n, q_hbm, k_hbm, v_hbm, o_ref, q_buf, k_buf, v_buf, s_buf, p_buf, sums, parts, stats, q_sem, k_sem, v_sem, piece_sem, send_sem, recv_sem):
    seqs, rows, head = k_hbm.shape
    heads = q_hbm.shape[1]
    tiles = rows // TILE
    log2e_scaled = math.log2(math.e) * head**-0.5
    me = lax.axis_index("sp")
    peers = list(peers_of(me))

    def k_copy(b):
        slot = lax.rem(b, K_SLOTS)
        return pltpu.make_async_copy(k_hbm.at[b], k_buf.at[slot], k_sem.at[slot])

    def v_copy(b):
        slot = lax.rem(b, V_SLOTS)
        return pltpu.make_async_copy(v_hbm.at[b], v_buf.at[slot], v_sem.at[slot])

    def piece_copy(i):
        part = pl.ds(i * (rows // PIECES), rows // PIECES)
        return pltpu.make_async_copy(v_hbm.at[seqs - 1, part], v_buf.at[(seqs - 1) % V_SLOTS, part], piece_sem.at[i])

    queue = [(k_copy, b) for b in range(LEAD + 1)]
    for b in range(seqs - LEAD - 1):
        queue += [(v_copy, b), (k_copy, b + LEAD + 1)]
    queue += [(v_copy, b) for b in range(seqs - LEAD - 1, seqs - 1)] + [(piece_copy, i) for i in range(PIECES)]
    last = len(queue) - PIECES

    def start(first):
        for copy, b in queue[first : first + 1] if first < last else queue[last:] if first == last else ():
            copy(b).start()

    def to(peer, ref, send, recv):
        return pltpu.make_async_remote_copy(
            src_ref=ref, dst_ref=ref, send_sem=send, recv_sem=recv, device_id={"sp": peer}, device_id_type=pl.DeviceIdType.MESH
        )

    pltpu.make_async_copy(q_hbm, q_buf, q_sem).start()
    for i in range(FLIGHT):
        start(i)

    barrier = pltpu.get_barrier_semaphore()
    for peer in peers:
        pl.semaphore_signal(barrier, inc=1, device_id={"sp": peer}, device_id_type=pl.DeviceIdType.MESH)

    own = lax.broadcasted_iota(jnp.int32, (heads, TILE), 1) % heads == lax.broadcasted_iota(jnp.int32, (heads, TILE), 0)
    lane = lax.broadcasted_iota(jnp.int32, (heads, LANES), 1)

    def score(b):
        slot = lax.rem(b, K_SLOTS)
        q = q_buf[b]
        for t in range(tiles):
            s = lax.dot_general(q, k_buf[slot, t * TILE : (t + 1) * TILE, :], (((1,), (1,)), ((), ())), preferred_element_type=jnp.float32)
            s_buf[:, t * TILE : (t + 1) * TILE] = jnp.where(own, s, -jnp.inf)

    def weigh(b, stat):
        p_slot = lax.rem(b, LEAD - 1)
        scores = [s_buf[:, t * TILE : (t + 1) * TILE] for t in range(tiles)]
        high = jnp.max(functools.reduce(jnp.maximum, scores), -1, keepdims=True)
        total = None
        for t in range(tiles):
            w = jnp.exp2((scores[t] - high) * log2e_scaled)
            p_buf[p_slot, :, t * TILE : (t + 1) * TILE] = w.astype(jnp.bfloat16)
            total = w if total is None else total + w
        total = jnp.sum(total, -1, keepdims=True)
        return jnp.where(lane == b, high, jnp.where(lane == b + LANES // 2, total, stat))

    def gather_values(b, sums, first, count):
        slot, p_slot = lax.rem(b, V_SLOTS), lax.rem(b, LEAD - 1)
        sums = list(sums)
        for t in range(first, first + count):
            d = jnp.dot(p_buf[p_slot, :, t * TILE : (t + 1) * TILE], v_buf[slot, t * TILE : (t + 1) * TILE, :], preferred_element_type=jnp.float32)
            i = t % len(sums)
            sums[i] = d if sums[i] is None else sums[i] + d
        return sums

    def keep(b, sums):
        parts[me, b] = sum(sums[1:], sums[0]).astype(jnp.bfloat16)

    def halves(b, first, count, i):
        for h in range(2):
            (sums[i + h],) = gather_values(b, [None], first + h * (count // 2), count // 2)

    def finish(b, count):
        first = me // n
        keep(b, [sums[first + i] for i in range(count)])

    pltpu.make_async_copy(q_hbm, q_buf, q_sem).wait()
    stat = jnp.zeros((heads, LANES), jnp.float32)
    for b in range(LEAD):
        k_copy(b).wait()
        start(FLIGHT + b)
        if b >= 1:
            stat = weigh(b - 1, stat)
        score(b)

    def step(b, stat):
        k_copy(b + LEAD).wait()
        if isinstance(b, int):
            start(LEAD + 2 * b + FLIGHT)
        elif FLIGHT % 2:
            v_copy(b + FLIGHT // 2).start()
        else:
            k_copy(b + LEAD + FLIGHT // 2).start()
        v_copy(b).wait()
        if isinstance(b, int):
            start(LEAD + 2 * b + FLIGHT + 1)
        elif FLIGHT % 2:
            k_copy(b + LEAD + FLIGHT // 2 + 1).start()
        else:
            v_copy(b + FLIGHT // 2).start()
        keep(b, gather_values(b, [None], 0, tiles))
        stat = weigh(b + LEAD - 1, stat)
        score(b + LEAD)
        return stat

    def send(first, count, k):
        for peer in peers:
            to(peer, parts.at[me, first : first + count], send_sem.at[k], recv_sem.at[k]).start()

    begin = 0
    for end in (seqs // 4, seqs // 2, 3 * seqs // 4 - 2, (last - FLIGHT) // 2 - LEAD):
        stat = lax.fori_loop(begin, end, step, stat)
        if begin == 0:
            pl.semaphore_wait(barrier, n - 1)
        send(begin, end - begin, 0)
        begin = end
    for b in range(begin, seqs - LEAD):
        stat = step(b, stat)
        send(b, 1, 0)
    for b in range(seqs - LEAD, seqs - 1):
        v_copy(b).wait()
        halves(b, 0, tiles, 0)
        if b == seqs - LEAD:
            stat = weigh(seqs - 1, stat)
            stats[me] = stat
        finish(b, 2)
        send(b, 1, 0)
        if b == seqs - LEAD:
            for peer in peers:
                to(peer, stats.at[me], send_sem.at[1], recv_sem.at[1]).start()
    for i in range(PIECES):
        piece_copy(i).wait()
        halves(seqs - 1, i * (tiles // PIECES), tiles // PIECES, 2 * i)
    finish(seqs - 1, 2 * PIECES)
    send(seqs - 1, 1, 2)

    to(peers[0], stats.at[0 : n - 1], send_sem.at[1], recv_sem.at[1]).wait()
    seen = [stats[i] for i in range(n)]
    high = functools.reduce(jnp.maximum, seen)
    scale = [jnp.exp2((s - high) * log2e_scaled) for s in seen]
    total = sum(c * pltpu.roll(s, LANES // 2, 1) for c, s in zip(scale, seen))
    scale = [c / total for c in scale]

    def weights_of(b):
        return [jnp.broadcast_to(c[:, b : b + 1], (heads, head)) for c in scale]

    def put(b, weights):
        o_ref[b] = sum(w * parts[i, b].astype(jnp.float32) for i, w in enumerate(weights)).astype(o_ref.dtype)

    to(peers[0], parts.at[0 : n - 1, 0 : seqs - 1], send_sem.at[0], recv_sem.at[0]).wait()
    for b in range(seqs - 1):
        put(b, weights_of(b))
    weights = weights_of(seqs - 1)
    to(peers[0], parts.at[0 : n - 1, 0], send_sem.at[2], recv_sem.at[2]).wait()
    put(seqs - 1, weights)


def solution(mesh):
    n = mesh.shape["sp"]

    def step(q, k, v):
        seqs, tokens, heads, head = k.shape
        rows = tokens * heads
        return pl.pallas_call(
            functools.partial(kernel, n),
            out_shape=pltpu.VMEM(q.shape, q.dtype),
            in_specs=[pl.BlockSpec(memory_space=pl.ANY)] * 3,
            out_specs=pl.BlockSpec(memory_space=pltpu.VMEM),
            scratch_shapes=[
                pltpu.VMEM(q.shape, q.dtype),
                pltpu.VMEM((K_SLOTS, rows, head), k.dtype),
                pltpu.VMEM((V_SLOTS, rows, head), v.dtype),
                pltpu.VMEM((heads, rows), jnp.float32),
                pltpu.VMEM((LEAD - 1, heads, rows), jnp.bfloat16),
                pltpu.VMEM((2 * PIECES, heads, head), jnp.float32),
                pltpu.VMEM((n, seqs, heads, head), jnp.bfloat16),
                pltpu.VMEM((n, heads, LANES), jnp.float32),
                pltpu.SemaphoreType.DMA,
                pltpu.SemaphoreType.DMA((K_SLOTS,)),
                pltpu.SemaphoreType.DMA((V_SLOTS,)),
                pltpu.SemaphoreType.DMA((PIECES,)),
                pltpu.SemaphoreType.DMA((3,)),
                pltpu.SemaphoreType.DMA((3,)),
            ],
            compiler_params=pltpu.CompilerParams(collective_id=0, has_side_effects=True),
        )(q, k.reshape(seqs, rows, head), v.reshape(seqs, rows, head))

    return jax.shard_map(
        step,
        mesh=mesh,
        in_specs=(P("dp", None, None), P("dp", "sp", None, None), P("dp", "sp", None, None)),
        out_specs=P("dp", None, None),
        check_vma=False,
    )
```

```python
import functools
import math

import jax
import jax.numpy as jnp
from jax import lax
from jax.experimental import pallas as pl
from jax.experimental.pallas import tpu as pltpu
from jax.sharding import PartitionSpec as P

K_SLOTS, V_SLOTS = 7, 7
FLIGHT = 8
LEAD = 4
LATE = 1
PIECES = (8, 4, 4)
TILE = 256
LANES = 128


def peers_of(me):
    x, y, core = me // 4, (me // 2) % 2, me % 2
    for dx, dy, dc in ((1, 1, 0), (1, 1, 1), (1, 0, 0), (1, 0, 1), (0, 1, 0), (0, 1, 1), (0, 0, 1)):
        px = 1 - x if dx else x
        py = 1 - y if dy else y
        pc = 1 - core if dc else core
        yield px * 4 + py * 2 + pc


def kernel(n, q_hbm, k_hbm, v_hbm, o_ref, q_buf, k_buf, v_buf, s_buf, p_buf, sums, parts, stats, q_sem, k_sem, v_sem, piece_sem, send_sem, recv_sem):
    seqs, rows, head = k_hbm.shape
    heads = q_hbm.shape[1]
    tiles = rows // TILE
    log2e_scaled = math.log2(math.e) * head**-0.5
    me = lax.axis_index("sp")
    peers = list(peers_of(me))

    def k_copy(b):
        slot = lax.rem(b, K_SLOTS)
        return pltpu.make_async_copy(k_hbm.at[b], k_buf.at[slot], k_sem.at[slot])

    def v_copy(b):
        slot = lax.rem(b, V_SLOTS)
        return pltpu.make_async_copy(v_hbm.at[b], v_buf.at[slot], v_sem.at[slot])

    def piece_copy(i):
        part = pl.ds(sum(PIECES[:i]) * TILE, PIECES[i] * TILE)
        return pltpu.make_async_copy(v_hbm.at[seqs - 1, part], v_buf.at[(seqs - 1) % V_SLOTS, part], piece_sem.at[i])

    queue = [(k_copy, b) for b in range(LEAD + 1)]
    for b in range(seqs - LEAD - 1):
        queue += [(v_copy, b), (k_copy, b + LEAD + 1)]
    queue += [(v_copy, b) for b in range(seqs - LEAD - 1, seqs - 1)] + [(piece_copy, i) for i in range(len(PIECES))]
    last = len(queue) - len(PIECES)

    def start(first):
        for copy, b in queue[first : first + 1] if first < last else queue[last:] if first == last else ():
            copy(b).start()

    def to(peer, ref, send, recv):
        return pltpu.make_async_remote_copy(
            src_ref=ref, dst_ref=ref, send_sem=send, recv_sem=recv, device_id={"sp": peer}, device_id_type=pl.DeviceIdType.MESH
        )

    start(0)
    pltpu.make_async_copy(q_hbm, q_buf, q_sem).start()
    for i in range(1, FLIGHT):
        start(i)

    barrier = pltpu.get_barrier_semaphore()
    for peer in peers:
        pl.semaphore_signal(barrier, inc=1, device_id={"sp": peer}, device_id_type=pl.DeviceIdType.MESH)

    own = lax.broadcasted_iota(jnp.int32, (heads, TILE), 1) % heads == lax.broadcasted_iota(jnp.int32, (heads, TILE), 0)
    lane = lax.broadcasted_iota(jnp.int32, (heads, LANES), 1)

    def score(b):
        slot = lax.rem(b, K_SLOTS)
        q = q_buf[b]
        for t in range(tiles):
            s = lax.dot_general(q, k_buf[slot, t * TILE : (t + 1) * TILE, :], (((1,), (1,)), ((), ())), preferred_element_type=jnp.float32)
            s_buf[:, t * TILE : (t + 1) * TILE] = jnp.where(own, s, -jnp.inf)

    def weigh(b, stat):
        p_slot = lax.rem(b, LEAD - 1)
        scores = [s_buf[:, t * TILE : (t + 1) * TILE] for t in range(tiles)]
        high = jnp.max(functools.reduce(jnp.maximum, scores), -1, keepdims=True)
        total = None
        for t in range(tiles):
            w = jnp.exp2((scores[t] - high) * log2e_scaled)
            p_buf[p_slot, :, t * TILE : (t + 1) * TILE] = w.astype(jnp.bfloat16)
            total = w if total is None else total + w
        total = jnp.sum(total, -1, keepdims=True)
        return jnp.where(lane == b, high, jnp.where(lane == b + LANES // 2, total, stat))

    def gather_values(b, first, count, total=None):
        slot, p_slot = lax.rem(b, V_SLOTS), lax.rem(b, LEAD - 1)
        for t in range(first, first + count):
            d = jnp.dot(p_buf[p_slot, :, t * TILE : (t + 1) * TILE], v_buf[slot, t * TILE : (t + 1) * TILE, :], preferred_element_type=jnp.float32)
            total = d if total is None else total + d
        return total

    def keep(b, total):
        parts[me, b] = total.astype(jnp.bfloat16)

    def keep_halves(b, pieces, before=lambda i: None):
        halves, begin = [None, None], 0
        for i, count in enumerate(pieces):
            before(i)
            for h in range(2):
                halves[h] = gather_values(b, begin + h * (count // 2), count // 2, halves[h])
            begin += count
        for h in range(2):
            sums[h] = halves[h]
        first = me // n
        keep(b, sums[first] + sums[first + 1])

    pltpu.make_async_copy(q_hbm, q_buf, q_sem).wait()
    stat = jnp.zeros((heads, LANES), jnp.float32)
    for b in range(LEAD):
        k_copy(b).wait()
        start(FLIGHT + b)
        if b >= 1:
            stat = weigh(b - 1, stat)
        score(b)

    def step(b, stat):
        k_copy(b + LEAD).wait()
        if isinstance(b, int):
            start(LEAD + 2 * b + FLIGHT)
        elif FLIGHT % 2:
            v_copy(b + FLIGHT // 2).start()
        else:
            k_copy(b + LEAD + FLIGHT // 2).start()
        v_copy(b).wait()
        if isinstance(b, int):
            start(LEAD + 2 * b + FLIGHT + 1)
        elif FLIGHT % 2:
            k_copy(b + LEAD + FLIGHT // 2 + 1).start()
        else:
            v_copy(b + FLIGHT // 2).start()
        keep(b, gather_values(b, 0, tiles))
        stat = weigh(b + LEAD - 1, stat)
        score(b + LEAD)
        return stat

    def place(b):
        return max(0, b - seqs + LATE + 1)

    def send(first, count, k):
        for peer in peers:
            to(peer, parts.at[me, pl.ds(first, count)], send_sem.at[0], recv_sem.at[k]).start()

    quiet, end = seqs // 4, (last - FLIGHT + 1) // 2 - LEAD
    stat = lax.fori_loop(0, quiet, step, stat)
    pl.semaphore_wait(barrier, n - 1)
    send(0, quiet, 0)

    def step_and_send(b, stat):
        stat = step(b, stat)
        send(b, 1, place(b) if isinstance(b, int) else 0)
        return stat

    stat = lax.fori_loop(quiet, end, step_and_send, stat)
    for b in range(end, seqs - LEAD):
        stat = step_and_send(b, stat)
    for b in range(seqs - LEAD, seqs - 1):
        v_copy(b).wait()
        keep_halves(b, (tiles,))
        if b == seqs - LEAD:
            stats[me] = weigh(seqs - 1, stat)
        send(b, 1, place(b))
        if b == seqs - LEAD:
            for peer in peers:
                to(peer, stats.at[me], send_sem.at[1], recv_sem.at[LATE + 1]).start()
    keep_halves(seqs - 1, PIECES, lambda i: piece_copy(i).wait())
    send(seqs - 1, 1, place(seqs - 1))

    to(peers[0], stats.at[0 : n - 1], send_sem.at[1], recv_sem.at[LATE + 1]).wait()
    seen = [stats[i] for i in range(n)]
    high = functools.reduce(jnp.maximum, seen)
    scale = [jnp.exp2((s - high) * log2e_scaled) for s in seen]
    total = sum(c * pltpu.roll(s, LANES // 2, 1) for c, s in zip(scale, seen))
    scale = [c / total for c in scale]

    def weights_of(b):
        return [jnp.broadcast_to(c[:, b : b + 1], (heads, head)) for c in scale]

    def put(b, weights):
        o_ref[b] = sum(w * parts[i, b].astype(jnp.float32) for i, w in enumerate(weights)).astype(o_ref.dtype)

    late = {b: weights_of(b) for b in range(seqs - LATE, seqs)}
    to(peers[0], parts.at[0 : n - 1, 0 : seqs - LATE], send_sem.at[0], recv_sem.at[0]).wait_recv()
    for b in range(seqs - LATE):
        put(b, weights_of(b))
    for b, weights in late.items():
        to(peers[0], parts.at[0 : n - 1, b], send_sem.at[0], recv_sem.at[place(b)]).wait_recv()
        put(b, weights)
    to(peers[0], parts.at[0 : n - 1], send_sem.at[0], recv_sem.at[0]).wait_send()


def solution(mesh):
    n = mesh.shape["sp"]

    def step(q, k, v):
        seqs, tokens, heads, head = k.shape
        rows = tokens * heads
        return pl.pallas_call(
            functools.partial(kernel, n),
            out_shape=pltpu.VMEM(q.shape, q.dtype),
            in_specs=[pl.BlockSpec(memory_space=pl.ANY)] * 3,
            out_specs=pl.BlockSpec(memory_space=pltpu.VMEM),
            scratch_shapes=[
                pltpu.VMEM(q.shape, q.dtype),
                pltpu.VMEM((K_SLOTS, rows, head), k.dtype),
                pltpu.VMEM((V_SLOTS, rows, head), v.dtype),
                pltpu.VMEM((heads, rows), jnp.float32),
                pltpu.VMEM((LEAD - 1, heads, rows), jnp.bfloat16),
                pltpu.VMEM((2, heads, head), jnp.float32),
                pltpu.VMEM((n, seqs, heads, head), jnp.bfloat16),
                pltpu.VMEM((n, heads, LANES), jnp.float32),
                pltpu.SemaphoreType.DMA,
                pltpu.SemaphoreType.DMA((K_SLOTS,)),
                pltpu.SemaphoreType.DMA((V_SLOTS,)),
                pltpu.SemaphoreType.DMA((len(PIECES),)),
                pltpu.SemaphoreType.DMA((2,)),
                pltpu.SemaphoreType.DMA((LATE + 2,)),
            ],
            compiler_params=pltpu.CompilerParams(collective_id=0, has_side_effects=True),
        )(q, k.reshape(seqs, rows, head), v.reshape(seqs, rows, head))

    return jax.shard_map(
        step,
        mesh=mesh,
        in_specs=(P("dp", None, None), P("dp", "sp", None, None), P("dp", "sp", None, None)),
        out_specs=P("dp", None, None),
        check_vma=False,
    )
```

```python
import functools
import math

import jax
import jax.numpy as jnp
from jax import lax
from jax.experimental import pallas as pl
from jax.experimental.pallas import tpu as pltpu
from jax.sharding import PartitionSpec as P

K_SLOTS, V_SLOTS = 6, 6
FLIGHT = 7
LEAD = 4
LATE = 1
PIECES = (8, 4, 4)
TILE = 256
LANES = 128


def peers_of(me):
    x, y, core = me // 4, (me // 2) % 2, me % 2
    for dx, dy, dc in ((1, 1, 0), (1, 1, 1), (1, 0, 0), (1, 0, 1), (0, 1, 0), (0, 1, 1), (0, 0, 1)):
        px = 1 - x if dx else x
        py = 1 - y if dy else y
        pc = 1 - core if dc else core
        yield px * 4 + py * 2 + pc


def kernel(n, q_hbm, k_hbm, v_hbm, o_ref, q_buf, k_buf, v_buf, s_buf, p_buf, sums, parts, stats, q_sem, k_sem, v_sem, piece_sem, send_sem, recv_sem):
    seqs, rows, head = k_hbm.shape
    heads = q_hbm.shape[1]
    tiles = rows // TILE
    log2e_scaled = math.log2(math.e) * head**-0.5
    me = lax.axis_index("sp")
    peers = list(peers_of(me))

    def k_copy(b):
        slot = lax.rem(b, K_SLOTS)
        return pltpu.make_async_copy(k_hbm.at[b], k_buf.at[slot], k_sem.at[slot])

    def v_copy(b):
        slot = lax.rem(b, V_SLOTS)
        return pltpu.make_async_copy(v_hbm.at[b], v_buf.at[slot], v_sem.at[slot])

    def piece_copy(i):
        part = pl.ds(sum(PIECES[:i]) * TILE, PIECES[i] * TILE)
        return pltpu.make_async_copy(v_hbm.at[seqs - 1, part], v_buf.at[(seqs - 1) % V_SLOTS, part], piece_sem.at[i])

    queue = [(k_copy, b) for b in range(LEAD + 1)]
    for b in range(seqs - LEAD - 1):
        queue += [(v_copy, b), (k_copy, b + LEAD + 1)]
    queue += [(v_copy, b) for b in range(seqs - LEAD - 1, seqs - 1)] + [(piece_copy, i) for i in range(len(PIECES))]
    last = len(queue) - len(PIECES)

    def start(first):
        for copy, b in queue[first : first + 1] if first < last else queue[last:] if first == last else ():
            copy(b).start()

    def to(peer, ref, send, recv):
        return pltpu.make_async_remote_copy(
            src_ref=ref, dst_ref=ref, send_sem=send, recv_sem=recv, device_id={"sp": peer}, device_id_type=pl.DeviceIdType.MESH
        )

    start(0)
    pltpu.make_async_copy(q_hbm, q_buf, q_sem).start()
    for i in range(1, FLIGHT):
        start(i)

    barrier = pltpu.get_barrier_semaphore()
    for peer in peers:
        pl.semaphore_signal(barrier, inc=1, device_id={"sp": peer}, device_id_type=pl.DeviceIdType.MESH)

    own = lax.broadcasted_iota(jnp.int32, (heads, TILE), 1) % heads == lax.broadcasted_iota(jnp.int32, (heads, TILE), 0)
    lane = lax.broadcasted_iota(jnp.int32, (heads, LANES), 1)

    def score(b):
        slot = lax.rem(b, K_SLOTS)
        q = q_buf[b]
        for t in range(tiles):
            s = lax.dot_general(q, k_buf[slot, t * TILE : (t + 1) * TILE, :], (((1,), (1,)), ((), ())), preferred_element_type=jnp.float32)
            s_buf[:, t * TILE : (t + 1) * TILE] = jnp.where(own, s, -jnp.inf)

    def weigh(b, stat):
        p_slot = lax.rem(b, LEAD - 1)
        scores = [s_buf[:, t * TILE : (t + 1) * TILE] for t in range(tiles)]
        high = jnp.max(functools.reduce(jnp.maximum, scores), -1, keepdims=True)
        total = None
        for t in range(tiles):
            w = jnp.exp2((scores[t] - high) * log2e_scaled)
            p_buf[p_slot, :, t * TILE : (t + 1) * TILE] = w.astype(jnp.bfloat16)
            total = w if total is None else total + w
        total = jnp.sum(total, -1, keepdims=True)
        return jnp.where(lane == b, high, jnp.where(lane == b + LANES // 2, total, stat))

    def gather_values(b, first, count, total=None):
        slot, p_slot = lax.rem(b, V_SLOTS), lax.rem(b, LEAD - 1)
        for t in range(first, first + count):
            d = jnp.dot(p_buf[p_slot, :, t * TILE : (t + 1) * TILE], v_buf[slot, t * TILE : (t + 1) * TILE, :], preferred_element_type=jnp.float32)
            total = d if total is None else total + d
        return total

    def keep(b, total):
        parts[me, b] = total.astype(jnp.bfloat16)

    def keep_halves(b, pieces, before=lambda i: None):
        halves, begin = [None, None], 0
        for i, count in enumerate(pieces):
            before(i)
            for h in range(2):
                halves[h] = gather_values(b, begin + h * (count // 2), count // 2, halves[h])
            begin += count
        for h in range(2):
            sums[h] = halves[h]
        first = me // n
        keep(b, sums[first] + sums[first + 1])

    pltpu.make_async_copy(q_hbm, q_buf, q_sem).wait()
    stat = jnp.zeros((heads, LANES), jnp.float32)
    for b in range(LEAD):
        k_copy(b).wait()
        start(FLIGHT + b)
        if b >= 1:
            stat = weigh(b - 1, stat)
        score(b)

    def step(b, stat):
        k_copy(b + LEAD).wait()
        if isinstance(b, int):
            start(LEAD + 2 * b + FLIGHT)
        elif FLIGHT % 2:
            v_copy(b + FLIGHT // 2).start()
        else:
            k_copy(b + LEAD + FLIGHT // 2).start()
        v_copy(b).wait()
        if isinstance(b, int):
            start(LEAD + 2 * b + FLIGHT + 1)
        elif FLIGHT % 2:
            k_copy(b + LEAD + FLIGHT // 2 + 1).start()
        else:
            v_copy(b + FLIGHT // 2).start()
        keep(b, gather_values(b, 0, tiles))
        stat = weigh(b + LEAD - 1, stat)
        score(b + LEAD)
        return stat

    def place(b):
        return max(0, b - seqs + LATE + 1)

    def send(first, count, k):
        for peer in peers:
            to(peer, parts.at[me, pl.ds(first, count)], send_sem.at[0], recv_sem.at[k]).start()

    quiet, end = seqs // 4, (last - FLIGHT + 1) // 2 - LEAD
    stat = lax.fori_loop(0, quiet, step, stat)
    pl.semaphore_wait(barrier, n - 1)
    send(0, quiet, 0)

    def step_and_send(b, stat):
        stat = step(b, stat)
        send(b, 1, place(b) if isinstance(b, int) else 0)
        return stat

    stat = lax.fori_loop(quiet, end, step_and_send, stat)
    for b in range(end, seqs - LEAD):
        stat = step_and_send(b, stat)
    for b in range(seqs - LEAD, seqs - 1):
        v_copy(b).wait()
        keep_halves(b, (tiles,))
        if b == seqs - LEAD:
            stats[me] = weigh(seqs - 1, stat)
        send(b, 1, place(b))
        if b == seqs - LEAD:
            for peer in peers:
                to(peer, stats.at[me], send_sem.at[1], recv_sem.at[LATE + 1]).start()
    keep_halves(seqs - 1, PIECES, lambda i: piece_copy(i).wait())
    send(seqs - 1, 1, place(seqs - 1))

    to(peers[0], stats.at[0 : n - 1], send_sem.at[1], recv_sem.at[LATE + 1]).wait()
    seen = [stats[i] for i in range(n)]
    high = functools.reduce(jnp.maximum, seen)
    scale = [jnp.exp2((s - high) * log2e_scaled) for s in seen]
    total = sum(c * pltpu.roll(s, LANES // 2, 1) for c, s in zip(scale, seen))
    scale = [c / total for c in scale]

    def weights_of(b):
        return [jnp.broadcast_to(c[:, b : b + 1], (heads, head)) for c in scale]

    def put(b, weights):
        o_ref[b] = sum(w * parts[i, b].astype(jnp.float32) for i, w in enumerate(weights)).astype(o_ref.dtype)

    late = {b: weights_of(b) for b in range(seqs - LATE, seqs)}
    to(peers[0], parts.at[0 : n - 1, 0 : seqs - LATE], send_sem.at[0], recv_sem.at[0]).wait_recv()
    for b in range(seqs - LATE):
        put(b, weights_of(b))
    for b, weights in late.items():
        to(peers[0], parts.at[0 : n - 1, b], send_sem.at[0], recv_sem.at[place(b)]).wait_recv()
        put(b, weights)
    to(peers[0], parts.at[0 : n - 1], send_sem.at[0], recv_sem.at[0]).wait_send()


def solution(mesh):
    n = mesh.shape["sp"]

    def step(q, k, v):
        seqs, tokens, heads, head = k.shape
        rows = tokens * heads
        return pl.pallas_call(
            functools.partial(kernel, n),
            out_shape=pltpu.VMEM(q.shape, q.dtype),
            in_specs=[pl.BlockSpec(memory_space=pl.ANY)] * 3,
            out_specs=pl.BlockSpec(memory_space=pltpu.VMEM),
            scratch_shapes=[
                pltpu.VMEM(q.shape, q.dtype),
                pltpu.VMEM((K_SLOTS, rows, head), k.dtype),
                pltpu.VMEM((V_SLOTS, rows, head), v.dtype),
                pltpu.VMEM((heads, rows), jnp.float32),
                pltpu.VMEM((LEAD - 1, heads, rows), jnp.bfloat16),
                pltpu.VMEM((2, heads, head), jnp.float32),
                pltpu.VMEM((n, seqs, heads, head), jnp.bfloat16),
                pltpu.VMEM((n, heads, LANES), jnp.float32),
                pltpu.SemaphoreType.DMA,
                pltpu.SemaphoreType.DMA((K_SLOTS,)),
                pltpu.SemaphoreType.DMA((V_SLOTS,)),
                pltpu.SemaphoreType.DMA((len(PIECES),)),
                pltpu.SemaphoreType.DMA((2,)),
                pltpu.SemaphoreType.DMA((LATE + 2,)),
            ],
            compiler_params=pltpu.CompilerParams(collective_id=0, has_side_effects=True),
        )(q, k.reshape(seqs, rows, head), v.reshape(seqs, rows, head))

    return jax.shard_map(
        step,
        mesh=mesh,
        in_specs=(P("dp", None, None), P("dp", "sp", None, None), P("dp", "sp", None, None)),
        out_specs=P("dp", None, None),
        check_vma=False,
    )
```
